32 devices in a mesh: occ: 8 (over z, y), aux: 4 (over x, core).
Axes of the slice: x: 2, y: 2, z: 4, core: 2. Of those that a mesh axis runs over, the one named last changes fastest.
Arguments:
- amplitudes: bfloat16 [2, 512, 2048], P(None, 'occ'), may hold values from -0.29882812 to 0.29882812
- fit_factor: bfloat16 [1024, 512, 2048], P('aux', 'occ'), may hold values from -0.14941406 to 0.14941406
Outputs:
- virtual_density: float32 [2, 2048, 2048], P(None, 'aux', 'occ')
- occupied_density: float32 [2, 512, 512], P(None, 'occ')
- right_side: float32 [2, 512, 2048], P(None, 'occ', 'aux')
The draws below stay inside these ranges and needn't reach their ends.
All inputs are finite; a program needn't handle non-finite values.
Results may differ from the reference program's by a relative error of at most 0.0068.
Values may be sent and summed in bfloat16 or wider, within the bound.
A program may use at most 128 MiB of HBM per device.

```python
import jax
import jax.numpy as jnp
from jax import lax

OCC = 512
VIRT = 2048
AUXF = 1024
STATES = 2


def block_levels(rng, shape, split, least, high):
    def one(dim, parts):
        heights = jax.random.uniform(jax.random.fold_in(jax.random.fold_in(rng, 6), dim), (parts,), jnp.float32, least / len(split), high / len(split))
        return jnp.repeat(jnp.exp(heights), shape[dim] // parts).reshape((-1,) + (1,) * (len(shape) - dim - 1))

    level = one(*split[0])
    for cut in split[1:]:
        level = level * one(*cut)
    return level


def scatter_about(own_key, extent, scale, limit, cuts=(), dtype=jnp.bfloat16):
    level = block_levels(own_key, extent, cuts, -0.22, 0.18) if cuts else 1.0
    entries = jax.random.normal(own_key, extent, jnp.float32) * scale * level
    return jnp.minimum(jnp.maximum(entries, -limit), limit).astype(dtype)


def setup_inputs(seed: int = 0) -> dict:
    seeds = jax.random.split(jax.random.key(seed), 3)
    amplitudes = scatter_about(seeds[0], (STATES, OCC, VIRT), 0.044, 0.29882812, ((1, 8),))
    fit_factor = scatter_about(seeds[1], (AUXF, OCC, VIRT), 0.023, 0.14941406, ((0, 4), (1, 8)))
    return dict(amplitudes=amplitudes, fit_factor=fit_factor)


def reference(amplitudes, fit_factor):
    wide = amplitudes.astype(jnp.float32)
    high = lax.Precision.HIGHEST
    virtual_density = jnp.einsum("sia,sib->sab", wide, wide, precision=high)
    occupied_density = jnp.einsum("sia,sja->sij", wide, wide, precision=high)
    flat_amp = amplitudes.reshape(STATES, OCC * VIRT)
    flat_fac = fit_factor.reshape(AUXF, OCC * VIRT)
    fitted = jnp.dot(flat_amp, flat_fac.T, preferred_element_type=jnp.float32).astype(jnp.bfloat16)
    field = jnp.dot(fitted, flat_fac, preferred_element_type=jnp.float32).astype(jnp.bfloat16)
    field_wide = field.reshape(STATES, OCC, VIRT).astype(jnp.float32)
    first = jnp.einsum("sib,sab->sia", field_wide, virtual_density, precision=high)
    second = jnp.einsum("sij,sja->sia", occupied_density, field_wide, precision=high)
    return virtual_density, occupied_density, first - second
```

```python
import functools

import jax
import jax.numpy as jnp
from jax import lax
from jax.experimental import pallas as pl
from jax.experimental.pallas import tpu as pltpu
from jax.sharding import PartitionSpec as P

F32 = jnp.float32
BF16 = jnp.bfloat16
NT = (((1,), (1,)), ((), ()))
MESH = pl.DeviceIdType.MESH
STAGES = 4
CHUNK = 16
BATCH = 64
RESIDENT_BYTES = 52 << 20


def split3(value):
    hi = value.astype(BF16)
    rest = value - hi.astype(F32)
    mid = rest.astype(BF16)
    return hi, mid, (rest - mid.astype(F32)).astype(BF16)


def field_kernel(
    loose, x_ref, b_ref, out_ref,
    held, spare, xs_ref, sums, spread, sel, parts, acc, own, sent, got,
    load_sem, spare_sem, fit_send, fit_recv, part_send, part_recv,
):
    states, rows, virt = x_ref.shape
    aux = b_ref.shape[0]
    n_occ, n_aux = lax.axis_size("occ"), lax.axis_size("aux")
    occ_at, aux_at = lax.axis_index("occ"), lax.axis_index("aux")
    slab = virt // n_aux
    width = slab // STAGES
    kept = aux - loose
    kept_chunks, loose_chunks = kept // CHUNK, loose // CHUNK
    depth = CHUNK * rows
    wide = states * rows

    def load(c):
        at = pl.ds(c * CHUNK, CHUNK)
        return pltpu.make_async_copy(b_ref.at[at], held.at[at], load_sem.at[c])

    def spare_loads(k):
        return [
            pltpu.make_async_copy(
                b_ref.at[pl.ds(kept, loose), :, pl.ds(u * slab + k * width, width)],
                spare.at[k % 2, :, :, pl.ds(u * width, width)],
                spare_sem.at[k, u],
            )
            for u in range(n_aux)
        ]

    if loose:
        for k in (3, 2):
            for copy in spare_loads(k):
                copy.start()
    for c in range(kept_chunks):
        load(c).start()

    barrier = pltpu.get_barrier_semaphore()
    for d in range(1, n_occ):
        pl.semaphore_signal(
            barrier, inc=1, device_id=(lax.rem(occ_at + d, n_occ), aux_at), device_id_type=MESH
        )
    for d in range(1, n_aux):
        pl.semaphore_signal(
            barrier, inc=1, device_id=(occ_at, lax.rem(aux_at + d, n_aux)), device_id_type=MESH
        )

    if loose:
        for k in range(STAGES):
            for u in range(n_aux):
                at = u * slab + k * width
                xs_ref[k, :, :, u * width : (u + 1) * width] = x_ref[:, :, at : at + width]
    row = lax.broadcasted_iota(jnp.int32, sel.shape, 0)
    col = lax.broadcasted_iota(jnp.int32, sel.shape, 1)
    sel[...] = jnp.where(lax.rem(row, CHUNK) == col // rows, 1.0, 0.0).astype(BF16)

    groups = 2 if rows % 32 == 0 else 1
    part = rows // groups
    pick_row = lax.broadcasted_iota(jnp.int32, (CHUNK, CHUNK * part), 0)
    pick_col = lax.broadcasted_iota(jnp.int32, (CHUNK, CHUNK * part), 1)
    pick = jnp.where(pick_col // part == pick_row, 1.0, 0.0).astype(BF16)

    def fit_terms(block, left):
        terms = [None] * states
        lanes = block.shape[2]
        step = min(lanes, 256)
        for at in range(0, lanes, step):
            cols = slice(at, at + step)
            for s in range(states):
                total = None
                for g in range(groups):
                    line = slice(g * part, (g + 1) * part)
                    term = block[:, line, cols] * left[s : s + 1, line, cols]
                    total = term if total is None else total + term
                value = jnp.dot(
                    pick, total.reshape(CHUNK * part, step), preferred_element_type=F32
                )
                for half in range(0, step, 128):
                    piece = value[:, half : half + 128]
                    terms[s] = piece if terms[s] is None else terms[s] + piece
        return terms

    def loose_fit(k):
        for copy in spare_loads(k):
            copy.wait()

        def step(c, carry):
            terms = fit_terms(spare.at[k % 2, pl.ds(c * CHUNK, CHUNK)], xs_ref.at[k])
            at = pl.ds(kept + c * CHUNK, CHUNK)
            for s in range(states):
                if k == STAGES - 1:
                    sums[s, at, :] = terms[s]
                else:
                    sums[s, at, :] += terms[s]
            return carry

        lax.fori_loop(0, loose_chunks, step, 0)

    if loose:
        for k in (3, 2):
            loose_fit(k)
            for copy in spare_loads(k - 2):
                copy.start()

    def kept_fit(c, carry):
        load(c).wait()
        at = pl.ds(c * CHUNK, CHUNK)
        terms = fit_terms(held.at[at], x_ref)
        for s in range(states):
            sums[s, at, :] = terms[s]
        return carry

    lax.fori_loop(0, kept_chunks, kept_fit, 0)
    if loose:
        for k in (1, 0):
            loose_fit(k)

    ones = jnp.ones((8, 128), BF16)
    for s in range(states):
        fit = sum(
            lax.dot_general(ones, piece, NT, preferred_element_type=F32)
            for piece in split3(sums[s])
        )
        parts[occ_at, s : s + 1] = fit[:1]
    pl.semaphore_wait(barrier, n_occ + n_aux - 2)

    def fit_copy(d):
        return pltpu.make_async_remote_copy(
            src_ref=parts.at[occ_at],
            dst_ref=parts.at[occ_at],
            send_sem=fit_send.at[d],
            recv_sem=fit_recv.at[d],
            device_id=(lax.rem(occ_at + d, n_occ), aux_at),
            device_id_type=MESH,
        )

    for d in range(1, n_occ):
        fit_copy(d).start()
    for d in range(1, n_occ):
        fit_copy(d).wait()
    total = parts[0]
    for j in range(1, n_occ):
        total += parts[j]
    fitted = total.astype(BF16).astype(F32)
    n_chunks = aux // CHUNK
    at_row = lax.broadcasted_iota(jnp.int32, (n_chunks, aux), 0)
    at_col = lax.broadcasted_iota(jnp.int32, (n_chunks, aux), 1)
    mine = at_col // CHUNK == at_row
    for s in range(states):
        picked = jnp.where(mine, jnp.broadcast_to(fitted[s : s + 1], (n_chunks, aux)), 0.0)
        spread[s] = jnp.dot(picked.astype(BF16), sel[...], preferred_element_type=F32)

    lane = lax.broadcasted_iota(jnp.int32, (rows, depth), 1)
    line = lax.broadcasted_iota(jnp.int32, (rows, depth), 0)
    keep = lax.rem(lane, rows) == line

    def left_of(c):
        blocks = [
            jnp.concatenate(
                [
                    jnp.where(keep, jnp.broadcast_to(spread[s, pl.ds(q, 1)], (rows, depth)), 0.0)
                    for s in range(states)
                ],
                axis=0,
            ).astype(BF16)
            for q in [c * (BATCH // CHUNK) + n for n in range(BATCH // CHUNK)]
        ]
        return jnp.concatenate(blocks, axis=1)

    def part_copy(k, d):
        return pltpu.make_async_remote_copy(
            src_ref=sent.at[k, d],
            dst_ref=got.at[k, d],
            send_sem=part_send.at[k, d],
            recv_sem=part_recv.at[k, d],
            device_id=(occ_at, lax.rem(aux_at + d, n_aux)),
            device_id_type=MESH,
        )

    def piece_of(d):
        at = pl.multiple_of(lax.rem(aux_at + d, n_aux) * width, width)
        return acc[:, pl.ds(at, width)]

    def finish(k):
        for d in range(1, n_aux):
            part_copy(k, d).wait()
        value = own[k]
        for d in range(1, n_aux):
            value += got[k, d].astype(F32)
        out_ref[:, :, k * width : (k + 1) * width] = value.astype(BF16).reshape(states, rows, width)

    for k in range(STAGES):
        acc[...] = jnp.zeros_like(acc)
        if loose and k >= 2:
            for copy in spare_loads(k):
                copy.wait()

        def kept_step(c, carry):
            at = pl.ds(c * BATCH, BATCH)
            block = jnp.concatenate(
                [
                    held[at, :, u * slab + k * width : u * slab + (k + 1) * width].reshape(
                        BATCH * rows, width
                    )
                    for u in range(n_aux)
                ],
                axis=1,
            )
            acc[...] += jnp.dot(left_of(c), block, preferred_element_type=F32)
            return carry

        def loose_step(c, carry):
            block = spare[k % 2, pl.ds(c * BATCH, BATCH)].reshape(BATCH * rows, n_aux * width)
            acc[...] += jnp.dot(left_of(kept // BATCH + c), block, preferred_element_type=F32)
            return carry

        if loose:
            lax.fori_loop(0, loose // BATCH, loose_step, 0)
            if k < 2:
                for copy in spare_loads(k + 2):
                    copy.start()
        lax.fori_loop(0, kept // BATCH, kept_step, 0)
        own[k] = piece_of(0)
        for d in range(1, n_aux):
            sent[k, d] = piece_of(d).astype(BF16)
        for d in range(1, n_aux):
            part_copy(k, d).start()
        if k:
            finish(k - 1)
    finish(STAGES - 1)


def field_cols_of(amplitudes, factor):
    n_occ, n_aux = lax.axis_size("occ"), lax.axis_size("aux")
    states, rows, virt = amplitudes.shape
    aux = factor.shape[0]
    slab = virt // n_aux
    width = slab // STAGES
    wide = states * rows
    loose = aux // 4 if aux * rows * virt * 2 > RESIDENT_BYTES else 0
    dma = pltpu.SemaphoreType.DMA
    return pl.pallas_call(
        functools.partial(field_kernel, loose),
        out_shape=jax.ShapeDtypeStruct((states, rows, slab), BF16),
        in_specs=[pl.BlockSpec(memory_space=pltpu.VMEM), pl.BlockSpec(memory_space=pl.ANY)],
        out_specs=pl.BlockSpec(memory_space=pltpu.VMEM),
        scratch_shapes=[
            pltpu.VMEM((aux - loose, rows, virt), BF16),
            pltpu.VMEM((2, max(loose, 8), rows, n_aux * width), BF16),
            pltpu.VMEM((STAGES, states, rows, n_aux * width), BF16),
            pltpu.VMEM((states, aux, 128), F32),
            pltpu.VMEM((states, aux // CHUNK, CHUNK * rows), F32),
            pltpu.VMEM((aux, CHUNK * rows), BF16),
            pltpu.VMEM((n_occ, states, aux), F32),
            pltpu.VMEM((wide, n_aux * width), F32),
            pltpu.VMEM((STAGES, wide, width), F32),
            pltpu.VMEM((STAGES, n_aux, wide, width), BF16),
            pltpu.VMEM((STAGES, n_aux, wide, width), BF16),
            dma(((aux - loose) // CHUNK,)),
            dma((STAGES, n_aux)),
            dma((n_occ,)),
            dma((n_occ,)),
            dma((STAGES, n_aux)),
            dma((STAGES, n_aux)),
        ],
        compiler_params=pltpu.CompilerParams(
            collective_id=0, has_side_effects=True, vmem_limit_bytes=67_043_328
        ),
        cost_estimate=pl.CostEstimate(
            flops=4 * wide * aux * rows * virt,
            bytes_accessed=2 * aux * rows * virt,
            transcendentals=0,
        ),
    )(amplitudes, factor)


def body(amplitudes, fit_factor):
    high = lax.Precision.HIGHEST
    slab = lax.axis_index("aux")
    width = amplitudes.shape[2] // lax.axis_size("aux")
    own_cols = lax.dynamic_slice_in_dim(amplitudes, slab * width, width, 2)
    gathered = lax.all_gather(own_cols, "occ", axis=1, tiled=True)
    blocked = lax.all_to_all(amplitudes, "occ", split_axis=2, concat_axis=1, tiled=True)
    virtual_density = jnp.einsum(
        "sia,sib->sab", gathered, blocked, preferred_element_type=jnp.float32
    )
    pair_part = jnp.einsum("sia,sja->sij", own_cols, gathered, preferred_element_type=jnp.float32)
    occupied_density = lax.psum(pair_part, "aux")
    field_cols = field_cols_of(amplitudes, fit_factor)
    second = jnp.einsum(
        "sij,sja->sia",
        occupied_density,
        lax.all_gather(field_cols, "occ", axis=1, tiled=True).astype(jnp.float32),
        precision=high,
    )
    cross_part = jnp.einsum(
        "sib,sjb->sij", field_cols, gathered, preferred_element_type=jnp.float32
    )
    cross = lax.psum(cross_part, "aux")
    first = jnp.einsum("sij,sja->sia", cross, gathered.astype(jnp.float32), precision=high)
    return (virtual_density, occupied_density, first - second)


def solution(mesh):
    placed = (P(None, "occ", None), P("aux", "occ", None))
    return jax.shard_map(
        body,
        mesh=mesh,
        in_specs=placed,
        out_specs=(P(None, "aux", "occ"), P(None, "occ", None), P(None, "occ", "aux")),
        check_vma=False,
    )
```

```python
import functools

import jax
import jax.numpy as jnp
from jax import lax
from jax.experimental import pallas as pl
from jax.experimental.pallas import tpu as pltpu
from jax.sharding import PartitionSpec as P

F32 = jnp.float32
BF16 = jnp.bfloat16
NT = (((1,), (1,)), ((), ()))
TN = (((0,), (0,)), ((), ()))
MESH = pl.DeviceIdType.MESH
STAGES = 4
CHUNK = 16
FIT = 16
BATCH = 64
RESIDENT_BYTES = 52 << 20


def split3(value):
    hi = value.astype(BF16)
    rest = value - hi.astype(F32)
    mid = rest.astype(BF16)
    return hi, mid, (rest - mid.astype(F32)).astype(BF16)


def wide_dot(left, right):
    hi, mid, _ = split3(left)
    return jnp.dot(hi, right, preferred_element_type=F32) + jnp.dot(
        mid, right, preferred_element_type=F32
    )


def densities_kernel(
    loose, x_ref, b_ref, vd_ref, od_ref, rs_ref,
    held, spare, xv, sums, spread, sel, parts, acc, own, sent, got,
    xs, xb, fg, od_part, od_got, od, cross, cross_out, vd, rs,
    load_sem, spare_sem, local_sem, fit_send, fit_recv, part_send, part_recv,
    xa_send, xa_recv, xf_send, xf_recv, xb_send, xb_recv, fa_send, fa_recv, ff_send, ff_recv,
    or_send, or_recv, oa_send, oa_recv, cr_send, cr_recv,
):
    states, rows, virt = x_ref.shape
    aux = b_ref.shape[0]
    n_occ, n_aux = lax.axis_size("occ"), lax.axis_size("aux")
    me, aux_at = lax.axis_index("occ"), lax.axis_index("aux")
    minor = 2 if n_occ % 2 == 0 else 1
    major = n_occ // minor
    row_at, side = me // minor, lax.rem(me, minor)
    slab = virt // n_aux
    width = slab // STAGES
    band = virt // n_occ
    block_w = xb.shape[2]
    occ = xs.shape[1]
    piece_w = occ // n_aux
    kept = aux - loose
    kept_chunks = kept // FIT
    depth = CHUNK * rows
    wide = states * rows
    slab_at = pl.multiple_of(aux_at * slab, slab)

    def lines(o):
        return pl.ds(pl.multiple_of(o * rows, rows), rows)

    def occ_peer(d):
        return lax.rem(me + d, n_occ), aux_at

    def aux_peer(d):
        return me, lax.rem(aux_at + d, n_aux)

    def far(d):
        return lax.rem(row_at + d, major) * minor + side, aux_at

    def near():
        return row_at * minor + (minor - 1 - side), aux_at

    def from_far(d):
        return lax.rem(row_at + major - d, major) * minor + side

    def remote(src, dst, send, recv, to):
        return pltpu.make_async_remote_copy(
            src_ref=src, dst_ref=dst, send_sem=send, recv_sem=recv, device_id=to, device_id_type=MESH
        )

    def load(c):
        at = pl.ds(c * FIT, FIT)
        return pltpu.make_async_copy(b_ref.at[at], held.at[at], load_sem.at[c])

    def spare_loads(k):
        return [
            pltpu.make_async_copy(
                b_ref.at[pl.ds(kept, loose), :, pl.ds(u * slab + k * width, width)],
                spare.at[k % 2, :, :, pl.ds(u * width, width)],
                spare_sem.at[k, u],
            )
            for u in range(n_aux)
        ]

    x_load = pltpu.make_async_copy(x_ref, xv, local_sem.at[0])
    own_cols = x_ref.at[:, :, pl.ds(slab_at, slab)]
    own_load = pltpu.make_async_copy(own_cols, xs.at[:, lines(me)], local_sem.at[1])
    x_load.start()
    if loose:
        for copy in spare_loads(3):
            copy.start()
    own_load.start()
    if loose:
        for copy in spare_loads(2):
            copy.start()
    for c in range(kept_chunks):
        load(c).start()

    barrier = pltpu.get_barrier_semaphore()
    for d in range(1, n_occ):
        pl.semaphore_signal(barrier, inc=1, device_id=occ_peer(d), device_id_type=MESH)
    for d in range(1, n_aux):
        pl.semaphore_signal(barrier, inc=1, device_id=aux_peer(d), device_id_type=MESH)

    row = lax.broadcasted_iota(jnp.int32, (CHUNK, depth), 0)
    col = lax.broadcasted_iota(jnp.int32, (CHUNK, depth), 1)
    pattern = jnp.where(row == col // rows, 1.0, 0.0).astype(BF16)
    for n in range(aux // CHUNK):
        sel[n * CHUNK : (n + 1) * CHUNK] = pattern
    pl.semaphore_wait(barrier, n_occ + n_aux - 2)

    def x_far(d):
        return remote(own_cols, xs.at[:, lines(me)], xa_send.at[d], xa_recv.at[d], far(d))

    def x_far_got(d):
        at = xs.at[:, lines(from_far(d))]
        return remote(at, at, xa_send.at[d], xa_recv.at[d], far(d))

    def x_near(d):
        at = xs.at[:, lines(from_far(d))]
        return remote(at if d else own_cols, at, xf_send.at[d], xf_recv.at[d], near())

    for d in range(1, major):
        x_far(d).start()
    if minor > 1:
        x_near(0).start()

    def x_forward(d):
        x_far_got(d).wait_recv()
        if minor > 1:
            x_near(d).start()

    fit_line = lax.broadcasted_iota(jnp.int32, (rows, wide), 0)
    fit_lane = lax.broadcasted_iota(jnp.int32, (rows, wide), 1)
    same = (lax.rem(fit_lane, rows) == fit_line)[None]

    def pair_sums(block, left):
        pairs = lax.dot_general(
            block.reshape(FIT * rows, left.shape[1]), left, NT, preferred_element_type=F32
        )
        return jnp.sum(jnp.where(same, pairs.reshape(FIT, rows, wide), 0.0), axis=1)

    def loose_fit(k):
        for copy in spare_loads(k):
            copy.wait()
        starts = [u * slab + k * width for u in range(n_aux)]

        def step(c, carry):
            left = jnp.concatenate([xv[:, :, a : a + width] for a in starts], axis=2)
            term = pair_sums(
                spare[k % 2, pl.ds(c * FIT, FIT)], left.reshape(wide, n_aux * width)
            )
            at = pl.ds(kept + c * FIT, FIT)
            if k == STAGES - 1:
                sums[at, :] = term
            else:
                sums[at, :] += term
            return carry

        lax.fori_loop(0, loose // FIT, step, 0)

    x_load.wait()
    if loose:
        for k in (3, 2):
            loose_fit(k)
            for copy in spare_loads(k - 2):
                copy.start()

    def kept_fit(c, carry):
        load(c).wait()
        at = pl.ds(c * FIT, FIT)
        sums[at, :] = pair_sums(held[at], xv[...].reshape(wide, virt))
        return carry

    done = 0
    for d in range(1, major):
        upto = kept_chunks * d // major
        lax.fori_loop(done, upto, kept_fit, 0)
        done = upto
        x_forward(d)
    lax.fori_loop(done, kept_chunks, kept_fit, 0)
    if loose:
        for k in (1, 0):
            loose_fit(k)

    ind_row = lax.broadcasted_iota(jnp.int32, (8, wide), 0)
    ind_col = lax.broadcasted_iota(jnp.int32, (8, wide), 1)
    ind = jnp.where(ind_col // rows == ind_row, 1.0, 0.0).astype(BF16)
    fit = sum(
        lax.dot_general(ind, piece, NT, preferred_element_type=F32) for piece in split3(sums[...])
    )
    parts[me] = fit[:states]

    def fit_copy(d):
        at = parts.at[me]
        return remote(at, at, fit_send.at[d], fit_recv.at[d], occ_peer(d))

    for d in range(1, n_occ):
        fit_copy(d).start()

    own_load.wait()
    if minor > 1:
        for d in range(major):
            x_near(d).wait_recv()
    for s in range(states):
        od_part[s] = lax.dot_general(xs[s, lines(me)], xs[s], NT, preferred_element_type=F32)

    def od_cols(u):
        return pl.ds(pl.multiple_of(u * piece_w, piece_w), piece_w)

    def od_reduce(d):
        to = aux_peer(d)
        return remote(od_part.at[:, :, od_cols(to[1])], od_got.at[d], or_send.at[d], or_recv.at[d], to)

    def od_share(d):
        at = od.at[:, :, od_cols(aux_at)]
        return remote(at, at, oa_send.at[d], oa_recv.at[d], aux_peer(d))

    for d in range(1, n_aux):
        od_reduce(d).start()

    holder = me * band // slab
    band_at = lax.rem(me * band, slab) // block_w * block_w
    band_cols = pl.ds(pl.multiple_of(band_at, block_w), block_w)
    mate = aux_at + 1 - 2 * lax.rem(aux_at, 2)
    along = lax.rem(aux_at, 2) == lax.rem(holder, 2)
    is_holder = aux_at == holder

    def band_copy(d, to):
        return remote(xs.at[:, :, band_cols], xb, xb_send.at[d], xb_recv, (me, to))

    relay = remote(xb, xb, xb_send.at[0], xb_recv, (me, mate))

    @pl.when(is_holder)
    def _():
        band_copy(0, mate).start()
        for d in range(2, n_aux, 2):
            band_copy(d, lax.rem(aux_at + d, n_aux)).start()
        xb[...] = xs[:, :, band_cols]

    for d in range(1, n_occ):
        fit_copy(d).wait()
    total = parts[0]
    for j in range(1, n_occ):
        total += parts[j]
    fitted = total.astype(BF16).astype(F32)
    n_chunks = aux // CHUNK
    at_row = lax.broadcasted_iota(jnp.int32, (n_chunks, aux), 0)
    at_col = lax.broadcasted_iota(jnp.int32, (n_chunks, aux), 1)
    mine = at_col // CHUNK == at_row
    for s in range(states):
        picked = jnp.where(mine, jnp.broadcast_to(fitted[s : s + 1], (n_chunks, aux)), 0.0)
        spread[s] = jnp.dot(picked.astype(BF16), sel[...], preferred_element_type=F32)

    lane = lax.broadcasted_iota(jnp.int32, (rows, depth), 1)
    line_at = lax.broadcasted_iota(jnp.int32, (rows, depth), 0)
    keep = lax.rem(lane, rows) == line_at

    def left_of(c):
        blocks = [
            jnp.concatenate(
                [
                    jnp.where(keep, jnp.broadcast_to(spread[s, pl.ds(q, 1)], (rows, depth)), 0.0)
                    for s in range(states)
                ],
                axis=0,
            ).astype(BF16)
            for q in [c * (BATCH // CHUNK) + n for n in range(BATCH // CHUNK)]
        ]
        return jnp.concatenate(blocks, axis=1)

    def part_copy(k, d):
        return remote(
            sent.at[k % 2, d], got.at[k, d], part_send.at[k, d], part_recv.at[k, d], aux_peer(d)
        )

    def piece_of(d):
        at = pl.multiple_of(lax.rem(aux_at + d, n_aux) * width, width)
        return acc[:, pl.ds(at, width)]

    def f_at(o, k):
        return fg.at[:, lines(o), pl.ds(k * width, width)]

    def f_far(k, d):
        at = f_at(me, k)
        return remote(at, at, fa_send.at[k, d], fa_recv.at[k, d], far(d))

    def f_far_got(k, d):
        at = f_at(from_far(d), k)
        return remote(at, at, fa_send.at[k, d], fa_recv.at[k, d], far(d))

    def f_near(k, d):
        at = f_at(from_far(d), k)
        return remote(at, at, ff_send.at[k, d], ff_recv.at[k, d], near())

    def finish(k):
        for d in range(1, n_aux):
            part_copy(k, d).wait()
        value = own[k % 2]
        for d in range(1, n_aux):
            value += got[k, d].astype(F32)
        value = value.astype(BF16).reshape(states, rows, width)
        fg[:, lines(me), k * width : (k + 1) * width] = value
        for d in range(1, major):
            f_far(k, d).start()
        if minor > 1:
            f_near(k, 0).start()
        for s in range(states):
            term = lax.dot_general(
                value[s], xs[s, :, k * width : (k + 1) * width], NT, preferred_element_type=F32
            )
            if k:
                cross[s] += term
            else:
                cross[s] = term

    def forward(k):
        for d in range(1, major):
            f_far_got(k, d).wait_recv()
            if minor > 1:
                f_near(k, d).start()

    def share_od():
        for d in range(1, n_aux):
            od_reduce(d).wait()
        value = od_part[:, :, od_cols(aux_at)]
        for d in range(1, n_aux):
            value += od_got[d]
        od[:, :, od_cols(aux_at)] = value
        for d in range(1, n_aux):
            od_share(d).start()

    for k in range(STAGES):
        acc[...] = jnp.zeros_like(acc)
        if loose and k >= 2:
            for copy in spare_loads(k):
                copy.wait()

        def kept_step(c, carry):
            at = pl.ds(c * BATCH, BATCH)
            block = jnp.concatenate(
                [
                    held[at, :, u * slab + k * width : u * slab + (k + 1) * width].reshape(
                        BATCH * rows, width
                    )
                    for u in range(n_aux)
                ],
                axis=1,
            )
            acc[...] += jnp.dot(left_of(c), block, preferred_element_type=F32)
            return carry

        def loose_step(c, carry):
            block = spare[k % 2, pl.ds(c * BATCH, BATCH)].reshape(BATCH * rows, n_aux * width)
            acc[...] += jnp.dot(left_of(kept // BATCH + c), block, preferred_element_type=F32)
            return carry

        if loose:
            lax.fori_loop(0, loose // BATCH, loose_step, 0)
            if k < 2:
                for copy in spare_loads(k + 2):
                    copy.start()
        lax.fori_loop(0, kept // BATCH - 1, kept_step, 0)
        if k:
            finish(k - 1)
        lax.fori_loop(kept // BATCH - 1, kept // BATCH, kept_step, 0)
        own[k % 2] = piece_of(0)
        for d in range(1, n_aux):
            sent[k % 2, d] = piece_of(d).astype(BF16)
        for d in range(1, n_aux):
            part_copy(k, d).start()
        if k == 0:
            share_od()
        if k >= 2:
            forward(k - 2)

    @pl.when(jnp.logical_not(is_holder))
    def _():
        relay.wait_recv()

        @pl.when(along)
        def _():
            relay.start()

    forward(STAGES - 2)
    finish(STAGES - 1)

    def cross_got(d):
        return held.at[pl.ds(d * states, states), :, pl.ds(0, occ)]

    def cross_copy(d):
        return remote(cross_out, cross_got(d), cr_send.at[d], cr_recv.at[d], aux_peer(d))

    cross_out[...] = cross[...].astype(BF16)
    for d in range(1, n_aux):
        cross_copy(d).start()

    vd_out = []
    for s in range(states):

        def vd_step(n, carry, s=s):
            at = pl.ds(pl.multiple_of(n * 128, 128), 128)
            value = lax.dot_general(xs[s, :, at], xb[s], TN, preferred_element_type=F32)
            if block_w > band:
                off = lax.rem(me * band, block_w)
                picked = value[:, :band]
                for m in range(1, block_w // band):
                    picked = jnp.where(off == m * band, value[:, m * band : (m + 1) * band], picked)
                value = picked
            vd[s, at] = value
            return carry

        lax.fori_loop(0, slab // 128, vd_step, 0)
        vd_out.append(pltpu.make_async_copy(vd.at[s], vd_ref.at[s], local_sem.at[2 + s]))
        vd_out[-1].start()

    forward(STAGES - 1)
    for d in range(1, n_aux):
        od_share(d).wait()
    od_out = pltpu.make_async_copy(od, od_ref, local_sem.at[0])
    od_out.start()
    for d in range(1, n_aux):
        cross_copy(d).wait()
    for s in range(states):
        total = cross[s]
        for d in range(1, n_aux):
            total += held[d * states + s, :, :occ].astype(F32)
        rs[s] = wide_dot(total, xs[s])
    if minor > 1:
        for k in range(STAGES):
            for d in range(major):
                f_near(k, d).wait_recv()
    for s in range(states):
        rs[s] = rs[s] - wide_dot(od[s], fg[s])
    rs_out = pltpu.make_async_copy(rs, rs_ref, local_sem.at[1])
    rs_out.start()

    for d in range(1, major):
        x_far(d).wait_send()
        for k in range(STAGES):
            f_far(k, d).wait_send()
    if minor > 1:
        for d in range(major):
            x_near(d).wait_send()
            for k in range(STAGES):
                f_near(k, d).wait_send()

    @pl.when(is_holder)
    def _():
        band_copy(0, mate).wait_send()
        for d in range(2, n_aux, 2):
            band_copy(d, lax.rem(aux_at + d, n_aux)).wait_send()

    @pl.when(jnp.logical_and(jnp.logical_not(is_holder), along))
    def _():
        relay.wait_send()

    for copy in vd_out:
        copy.wait()
    od_out.wait()
    rs_out.wait()


def body(amplitudes, factor):
    n_occ, n_aux = lax.axis_size("occ"), lax.axis_size("aux")
    states, rows, virt = amplitudes.shape
    aux = factor.shape[0]
    occ = rows * n_occ
    slab = virt // n_aux
    width = slab // STAGES
    band = virt // n_occ
    block_w = max(band, 128)
    wide = states * rows
    loose = aux // 4 if aux * rows * virt * 2 > RESIDENT_BYTES else 0
    major = n_occ // (2 if n_occ % 2 == 0 else 1)
    dma = pltpu.SemaphoreType.DMA
    whole = pl.BlockSpec(memory_space=pl.ANY)
    return pl.pallas_call(
        functools.partial(densities_kernel, loose),
        out_shape=(
            jax.ShapeDtypeStruct((states, slab, band), F32),
            jax.ShapeDtypeStruct((states, rows, occ), F32),
            jax.ShapeDtypeStruct((states, rows, slab), F32),
        ),
        in_specs=[whole] * 2,
        out_specs=(whole,) * 3,
        scratch_shapes=[
            pltpu.VMEM((aux - loose, rows, virt), BF16),
            pltpu.VMEM((2, max(loose, 8), rows, n_aux * width), BF16),
            pltpu.VMEM((states, rows, virt), BF16),
            pltpu.VMEM((aux, wide), F32),
            pltpu.VMEM((states, aux // CHUNK, CHUNK * rows), F32),
            pltpu.VMEM((aux, CHUNK * rows), BF16),
            pltpu.VMEM((n_occ, states, aux), F32),
            pltpu.VMEM((wide, n_aux * width), F32),
            pltpu.VMEM((2, wide, width), F32),
            pltpu.VMEM((2, n_aux, wide, width), BF16),
            pltpu.VMEM((STAGES, n_aux, wide, width), BF16),
            pltpu.VMEM((states, occ, slab), BF16),
            pltpu.VMEM((states, occ, block_w), BF16),
            pltpu.VMEM((states, occ, slab), BF16),
            pltpu.VMEM((states, rows, occ), F32),
            pltpu.VMEM((n_aux, states, rows, occ // n_aux), F32),
            pltpu.VMEM((states, rows, occ), F32),
            pltpu.VMEM((states, rows, occ), F32),
            pltpu.VMEM((states, rows, occ), BF16),
            pltpu.VMEM((states, slab, band), F32),
            pltpu.VMEM((states, rows, slab), F32),
            dma(((aux - loose) // FIT,)),
            dma((STAGES, n_aux)),
            dma((2 + states,)),
            dma((n_occ,)),
            dma((n_occ,)),
            dma((STAGES, n_aux)),
            dma((STAGES, n_aux)),
            dma((major,)),
            dma((major,)),
            dma((major,)),
            dma((major,)),
            dma((n_aux,)),
            dma(()),
            dma((STAGES, major)),
            dma((STAGES, major)),
            dma((STAGES, major)),
            dma((STAGES, major)),
            dma((n_aux,)),
            dma((n_aux,)),
            dma((n_aux,)),
            dma((n_aux,)),
            dma((n_aux,)),
            dma((n_aux,)),
        ],
        compiler_params=pltpu.CompilerParams(
            collective_id=0, has_side_effects=True, vmem_limit_bytes=67_043_328
        ),
        cost_estimate=pl.CostEstimate(
            flops=4 * wide * aux * rows * virt,
            bytes_accessed=2 * aux * rows * virt,
            transcendentals=0,
        ),
    )(amplitudes, factor)


def solution(mesh):
    placed = (P(None, "occ", None), P("aux", "occ", None))
    return jax.shard_map(
        body,
        mesh=mesh,
        in_specs=placed,
        out_specs=(P(None, "aux", "occ"), P(None, "occ", None), P(None, "occ", "aux")),
        check_vma=False,
    )
```

```python
import functools

import jax
import jax.numpy as jnp
from jax import lax
from jax.experimental import pallas as pl
from jax.experimental.pallas import tpu as pltpu
from jax.sharding import PartitionSpec as P

F32 = jnp.float32
BF16 = jnp.bfloat16
NT = (((1,), (1,)), ((), ()))
TN = (((0,), (0,)), ((), ()))
MESH = pl.DeviceIdType.MESH
STAGES = 4
CHUNK = 16
FIT = 16
LOOSE_FIT = 32
AHEAD = 4
BATCH = 64
RESIDENT_BYTES = 52 << 20


def split3(value):
    hi = value.astype(BF16)
    rest = value - hi.astype(F32)
    mid = rest.astype(BF16)
    return hi, mid, (rest - mid.astype(F32)).astype(BF16)


def wide_dot(left, right):
    hi, mid, _ = split3(left)
    return jnp.dot(hi, right, preferred_element_type=F32) + jnp.dot(
        mid, right, preferred_element_type=F32
    )


def densities_kernel(
    loose, x_ref, b_ref, vd_ref, od_ref, rs_ref,
    held, spare, xv, sums, spread, sel, parts, acc, own, sent, got,
    xs, xb, fg, od_part, od_got, od, cross, cross_out, vd, rs,
    load_sem, spare_sem, local_sem, fit_send, fit_recv, part_send, part_recv,
    xa_send, xa_recv, xf_send, xf_recv, xb_send, xb_recv, fa_send, fa_recv, ff_send, ff_recv,
    or_send, or_recv, oa_send, oa_recv, cr_send, cr_recv,
):
    states, rows, virt = x_ref.shape
    aux = b_ref.shape[0]
    n_occ, n_aux = lax.axis_size("occ"), lax.axis_size("aux")
    me, aux_at = lax.axis_index("occ"), lax.axis_index("aux")
    minor = 2 if n_occ % 2 == 0 else 1
    major = n_occ // minor
    row_at, side = me // minor, lax.rem(me, minor)
    slab = virt // n_aux
    width = slab // STAGES
    band = virt // n_occ
    block_w = xb.shape[2]
    occ = xs.shape[1]
    piece_w = occ // n_aux
    kept = aux - loose
    kept_chunks = kept // FIT
    depth = CHUNK * rows
    wide = states * rows
    slab_at = pl.multiple_of(aux_at * slab, slab)

    def lines(o):
        return pl.ds(pl.multiple_of(o * rows, rows), rows)

    def occ_peer(d):
        return lax.rem(me + d, n_occ), aux_at

    def aux_peer(d):
        return me, lax.rem(aux_at + d, n_aux)

    def far(d):
        return lax.rem(row_at + d, major) * minor + side, aux_at

    def near():
        return row_at * minor + (minor - 1 - side), aux_at

    def from_far(d):
        return lax.rem(row_at + major - d, major) * minor + side

    def remote(src, dst, send, recv, to):
        return pltpu.make_async_remote_copy(
            src_ref=src, dst_ref=dst, send_sem=send, recv_sem=recv, device_id=to, device_id_type=MESH
        )

    def load(c):
        at = pl.ds(c * FIT, FIT)
        return pltpu.make_async_copy(b_ref.at[at], held.at[at], load_sem.at[c % AHEAD])

    def spare_loads(k):
        return [
            pltpu.make_async_copy(
                b_ref.at[pl.ds(kept, loose), :, pl.ds(u * slab + k * width, width)],
                spare.at[k % 2, :, :, pl.ds(u * width, width)],
                spare_sem.at[k % 2, u],
            )
            for u in range(n_aux)
        ]

    x_load = pltpu.make_async_copy(x_ref, xv, local_sem.at[0])
    own_cols = x_ref.at[:, :, pl.ds(slab_at, slab)]
    own_load = pltpu.make_async_copy(own_cols, xs.at[:, lines(me)], local_sem.at[1])
    x_load.start()
    ahead = min(AHEAD, kept_chunks)
    lead = 2 if loose else 0
    for c in range(lead or ahead):
        load(c).start()
    own_load.start()
    if loose:
        for k in (3, 2):
            for copy in spare_loads(k):
                copy.start()

    barrier = pltpu.get_barrier_semaphore()
    for d in range(1, n_occ):
        pl.semaphore_signal(barrier, inc=1, device_id=occ_peer(d), device_id_type=MESH)
    for d in range(1, n_aux):
        pl.semaphore_signal(barrier, inc=1, device_id=aux_peer(d), device_id_type=MESH)

    row = lax.broadcasted_iota(jnp.int32, (CHUNK, depth), 0)
    col = lax.broadcasted_iota(jnp.int32, (CHUNK, depth), 1)
    pattern = jnp.where(row == col // rows, 1.0, 0.0).astype(BF16)
    for n in range(aux // CHUNK):
        sel[n * CHUNK : (n + 1) * CHUNK] = pattern
    pl.semaphore_wait(barrier, n_occ + n_aux - 2)

    def x_far(d):
        return remote(own_cols, xs.at[:, lines(me)], xa_send.at[d], xa_recv.at[d], far(d))

    def x_far_got(d):
        at = xs.at[:, lines(from_far(d))]
        return remote(at, at, xa_send.at[d], xa_recv.at[d], far(d))

    def x_near(d):
        at = xs.at[:, lines(from_far(d))]
        return remote(at if d else own_cols, at, xf_send.at[d], xf_recv.at[d], near())

    for d in range(1, major):
        x_far(d).start()
    if minor > 1:
        x_near(0).start()

    def x_forward(d):
        x_far_got(d).wait_recv()
        if minor > 1:
            x_near(d).start()

    fit_line = lax.broadcasted_iota(jnp.int32, (rows, wide), 0)
    fit_lane = lax.broadcasted_iota(jnp.int32, (rows, wide), 1)
    same = (lax.rem(fit_lane, rows) == fit_line)[None]

    def pair_sums(block, left):
        pairs = lax.dot_general(
            block.reshape(block.shape[0] * rows, left.shape[1]), left, NT, preferred_element_type=F32
        )
        return jnp.sum(jnp.where(same, pairs.reshape(block.shape[0], rows, wide), 0.0), axis=1)

    def loose_fit(k):
        for copy in spare_loads(k):
            copy.wait()
        starts = [u * slab + k * width for u in range(n_aux)]

        def step(c, carry):
            left = jnp.concatenate([xv[:, :, a : a + width] for a in starts], axis=2)
            term = pair_sums(
                spare[k % 2, pl.ds(c * LOOSE_FIT, LOOSE_FIT)], left.reshape(wide, n_aux * width)
            )
            at = pl.ds(kept + c * LOOSE_FIT, LOOSE_FIT)
            if k == STAGES - 1:
                sums[at, :] = term
            else:
                sums[at, :] += term
            return carry

        lax.fori_loop(0, loose // LOOSE_FIT, step, 0)

    ind_row = lax.broadcasted_iota(jnp.int32, (8, wide), 0)
    ind_col = lax.broadcasted_iota(jnp.int32, (8, wide), 1)
    ind = jnp.where(ind_col // rows == ind_row, 1.0, 0.0).astype(BF16)
    spans = [(0, kept), (kept, loose)]

    def fit_copy(g, d):
        at = parts.at[g, me]
        return remote(at, at, fit_send.at[g, d], fit_recv.at[g, d], occ_peer(d))

    def send_fit(g):
        start, size = spans[g]
        pieces = split3(sums[start : start + size])
        fit = sum(lax.dot_general(ind, p, NT, preferred_element_type=F32) for p in pieces)
        parts[g, me] = jnp.zeros((states, aux), F32)
        parts[g, me, :, :size] = fit[:states]
        for d in range(1, n_occ):
            fit_copy(g, d).start()

    def spread_fit(g):
        start, size = spans[g]
        for d in range(1, n_occ):
            fit_copy(g, d).wait()
        total = parts[g, 0, :, :size]
        for j in range(1, n_occ):
            total += parts[g, j, :, :size]
        fitted = total.astype(BF16).astype(F32)
        chunks = size // CHUNK
        at_row = lax.broadcasted_iota(jnp.int32, (chunks, size), 0)
        at_col = lax.broadcasted_iota(jnp.int32, (chunks, size), 1)
        first = start // CHUNK
        for s in range(states):
            picked = jnp.where(
                at_col // CHUNK == at_row, jnp.broadcast_to(fitted[s : s + 1], (chunks, size)), 0.0
            )
            spread[s, first : first + chunks] = jnp.dot(
                picked.astype(BF16), sel[:size], preferred_element_type=F32
            )

    x_load.wait()
    def kept_sum(c):
        at = pl.ds(c * FIT, FIT)
        sums[at, :] = pair_sums(held[at], xv[...].reshape(wide, virt))

    def kept_fit(c, carry):
        load(c).wait()

        @pl.when(c + ahead < kept_chunks)
        def _():
            load(c + ahead).start()

        kept_sum(c)
        return carry

    def lead_fit(c, carry):
        load(c).wait()
        load(c + lead).start()
        kept_sum(c)
        return carry

    if loose:
        lax.fori_loop(0, lead, lead_fit, 0)
        for k in (3, 2):
            loose_fit(k)
            load(2 * lead + 3 - k).start()

    done = lead
    for d in range(1, major):
        upto = lead + (kept_chunks - lead) * d // major
        lax.fori_loop(done, upto, kept_fit, 0)
        done = upto
        x_forward(d)
    if loose:
        for k in (1, 0):
            for copy in spare_loads(k):
                copy.start()
    lax.fori_loop(done, kept_chunks, kept_fit, 0)
    send_fit(0)

    own_load.wait()
    if minor > 1:
        for d in range(major):
            x_near(d).wait_recv()
    for s in range(states):
        od_part[s] = lax.dot_general(xs[s, lines(me)], xs[s], NT, preferred_element_type=F32)

    def od_cols(u):
        return pl.ds(pl.multiple_of(u * piece_w, piece_w), piece_w)

    def od_reduce(d):
        to = aux_peer(d)
        return remote(od_part.at[:, :, od_cols(to[1])], od_got.at[d], or_send.at[d], or_recv.at[d], to)

    def od_share(d):
        at = od.at[:, :, od_cols(aux_at)]
        return remote(at, at, oa_send.at[d], oa_recv.at[d], aux_peer(d))

    for d in range(1, n_aux):
        od_reduce(d).start()

    holder = me * band // slab
    band_at = lax.rem(me * band, slab) // block_w * block_w
    band_cols = pl.ds(pl.multiple_of(band_at, block_w), block_w)
    mate = aux_at + 1 - 2 * lax.rem(aux_at, 2)
    along = lax.rem(aux_at, 2) == lax.rem(holder, 2)
    is_holder = aux_at == holder

    def band_copy(d, to):
        return remote(xs.at[:, :, band_cols], xb, xb_send.at[d], xb_recv, (me, to))

    relay = remote(xb, xb, xb_send.at[0], xb_recv, (me, mate))

    @pl.when(is_holder)
    def _():
        band_copy(0, mate).start()
        for d in range(2, n_aux, 2):
            band_copy(d, lax.rem(aux_at + d, n_aux)).start()
        xb[...] = xs[:, :, band_cols]

    if loose:
        for k in (1, 0):
            loose_fit(k)

    if loose:
        send_fit(1)

    spread_fit(0)
    lane = lax.broadcasted_iota(jnp.int32, (rows, depth), 1)
    line_at = lax.broadcasted_iota(jnp.int32, (rows, depth), 0)
    keep = lax.rem(lane, rows) == line_at

    def left_of(c):
        blocks = [
            jnp.concatenate(
                [
                    jnp.where(keep, jnp.broadcast_to(spread[s, pl.ds(q, 1)], (rows, depth)), 0.0)
                    for s in range(states)
                ],
                axis=0,
            ).astype(BF16)
            for q in [c * (BATCH // CHUNK) + n for n in range(BATCH // CHUNK)]
        ]
        return jnp.concatenate(blocks, axis=1)

    def part_copy(k, d):
        return remote(
            sent.at[k % 2, d], got.at[k, d], part_send.at[k, d], part_recv.at[k, d], aux_peer(d)
        )

    def piece_of(d):
        at = pl.multiple_of(lax.rem(aux_at + d, n_aux) * width, width)
        return acc[:, pl.ds(at, width)]

    def f_at(o, k):
        return fg.at[:, lines(o), pl.ds(k * width, width)]

    def f_far(k, d):
        at = f_at(me, k)
        return remote(at, at, fa_send.at[k, d], fa_recv.at[k, d], far(d))

    def f_far_got(k, d):
        at = f_at(from_far(d), k)
        return remote(at, at, fa_send.at[k, d], fa_recv.at[k, d], far(d))

    def f_near(k, d):
        at = f_at(from_far(d), k)
        return remote(at, at, ff_send.at[k, d], ff_recv.at[k, d], near())

    def finish(k):
        for d in range(1, n_aux):
            part_copy(k, d).wait()
        value = own[k % 2]
        for d in range(1, n_aux):
            value += got[k, d].astype(F32)
        value = value.astype(BF16).reshape(states, rows, width)
        fg[:, lines(me), k * width : (k + 1) * width] = value
        for d in range(1, major):
            f_far(k, d).start()
        if minor > 1:
            f_near(k, 0).start()
        for s in range(states):
            term = lax.dot_general(
                value[s], xs[s, :, k * width : (k + 1) * width], NT, preferred_element_type=F32
            )
            if k:
                cross[s] += term
            else:
                cross[s] = term

    def forward(k):
        for d in range(1, major):
            f_far_got(k, d).wait_recv()
            if minor > 1:
                f_near(k, d).start()

    def share_od():
        for d in range(1, n_aux):
            od_reduce(d).wait()
        value = od_part[:, :, od_cols(aux_at)]
        for d in range(1, n_aux):
            value += od_got[d]
        od[:, :, od_cols(aux_at)] = value
        for d in range(1, n_aux):
            od_share(d).start()

    for k in range(STAGES):
        acc[...] = jnp.zeros_like(acc)
        if loose and k >= 2:
            for copy in spare_loads(k):
                copy.wait()

        def kept_step(c, carry):
            at = pl.ds(c * BATCH, BATCH)
            block = jnp.concatenate(
                [
                    held[at, :, u * slab + k * width : u * slab + (k + 1) * width].reshape(
                        BATCH * rows, width
                    )
                    for u in range(n_aux)
                ],
                axis=1,
            )
            acc[...] += jnp.dot(left_of(c), block, preferred_element_type=F32)
            return carry

        def loose_step(c, carry):
            block = spare[k % 2, pl.ds(c * BATCH, BATCH)].reshape(BATCH * rows, n_aux * width)
            acc[...] += jnp.dot(left_of(kept // BATCH + c), block, preferred_element_type=F32)
            return carry

        if k == 0:
            lax.fori_loop(0, kept // BATCH, kept_step, 0)
            if loose:
                spread_fit(1)
        if loose:
            lax.fori_loop(0, loose // BATCH, loose_step, 0)
            if k < 2:
                for copy in spare_loads(k + 2):
                    copy.start()
        if k:
            lax.fori_loop(0, kept // BATCH, kept_step, 0)
        own[k % 2] = piece_of(0)
        for d in range(1, n_aux):
            sent[k % 2, d] = piece_of(d).astype(BF16)
        for d in range(1, n_aux):
            part_copy(k, d).start()
        if k:
            finish(k - 1)
        if k == 1:
            share_od()
        if k >= 2:
            forward(k - 2)

    @pl.when(jnp.logical_not(is_holder))
    def _():
        relay.wait_recv()

        @pl.when(along)
        def _():
            relay.start()

    vd_out = []
    for s in range(states):

        def vd_step(n, carry, s=s):
            at = pl.ds(pl.multiple_of(n * 128, 128), 128)
            value = lax.dot_general(xs[s, :, at], xb[s], TN, preferred_element_type=F32)
            if block_w > band:
                off = lax.rem(me * band, block_w)
                picked = value[:, :band]
                for m in range(1, block_w // band):
                    picked = jnp.where(off == m * band, value[:, m * band : (m + 1) * band], picked)
                value = picked
            vd[s, at] = value
            return carry

        lax.fori_loop(0, slab // 128, vd_step, 0)
        vd_out.append(pltpu.make_async_copy(vd.at[s], vd_ref.at[s], local_sem.at[2 + s]))
        vd_out[-1].start()

    finish(STAGES - 1)

    def cross_got(d):
        return held.at[pl.ds(d * states, states), :, pl.ds(0, occ)]

    def cross_copy(d):
        return remote(cross_out, cross_got(d), cr_send.at[d], cr_recv.at[d], aux_peer(d))

    cross_out[...] = cross[...].astype(BF16)
    for d in range(1, n_aux):
        cross_copy(d).start()

    forward(STAGES - 2)
    forward(STAGES - 1)
    for d in range(1, n_aux):
        od_share(d).wait()
    od_out = pltpu.make_async_copy(od, od_ref, local_sem.at[0])
    od_out.start()
    for d in range(1, n_aux):
        cross_copy(d).wait()
    for s in range(states):
        total = cross[s]
        for d in range(1, n_aux):
            total += held[d * states + s, :, :occ].astype(F32)
        rs[s] = wide_dot(total, xs[s])
    if minor > 1:
        for k in range(STAGES):
            for d in range(major):
                f_near(k, d).wait_recv()
    for s in range(states):
        rs[s] = rs[s] - wide_dot(od[s], fg[s])
    rs_out = pltpu.make_async_copy(rs, rs_ref, local_sem.at[1])
    rs_out.start()

    for d in range(1, major):
        x_far(d).wait_send()
        for k in range(STAGES):
            f_far(k, d).wait_send()
    if minor > 1:
        for d in range(major):
            x_near(d).wait_send()
            for k in range(STAGES):
                f_near(k, d).wait_send()

    @pl.when(is_holder)
    def _():
        band_copy(0, mate).wait_send()
        for d in range(2, n_aux, 2):
            band_copy(d, lax.rem(aux_at + d, n_aux)).wait_send()

    @pl.when(jnp.logical_and(jnp.logical_not(is_holder), along))
    def _():
        relay.wait_send()

    for copy in vd_out:
        copy.wait()
    od_out.wait()
    rs_out.wait()


def results_kernel(*refs):
    count = len(refs) // 3
    given, results, held = refs[:count], refs[count : 2 * count], refs[2 * count : 3 * count]
    sems = refs[3 * count]
    spans = [(n, s) for n in range(count) for s in range(given[n].shape[0])]
    ins, outs = [], []
    for at, (n, s) in enumerate(spans):
        ins.append(pltpu.make_async_copy(given[n].at[s], held[n].at[s], sems.at[at, 0]))
        outs.append(pltpu.make_async_copy(held[n].at[s], results[n].at[s], sems.at[at, 1]))
    for copy in ins:
        copy.start()
    for at in range(len(spans)):
        ins[at].wait()
        outs[at].start()
    for copy in outs:
        copy.wait()


def write_results(*given):
    whole = pl.BlockSpec(memory_space=pl.ANY)
    count = len(given)
    return pl.pallas_call(
        results_kernel,
        out_shape=tuple(jax.ShapeDtypeStruct(g.shape, g.dtype) for g in given),
        in_specs=[whole] * count,
        out_specs=(whole,) * count,
        scratch_shapes=[
            *[pltpu.VMEM(g.shape, g.dtype) for g in given],
            pltpu.SemaphoreType.DMA((sum(g.shape[0] for g in given), 2)),
        ],
        cost_estimate=pl.CostEstimate(
            flops=0, bytes_accessed=2 * sum(g.size * 4 for g in given), transcendentals=0
        ),
    )(*given)


def body(amplitudes, factor):
    n_occ, n_aux = lax.axis_size("occ"), lax.axis_size("aux")
    states, rows, virt = amplitudes.shape
    aux = factor.shape[0]
    occ = rows * n_occ
    slab = virt // n_aux
    width = slab // STAGES
    band = virt // n_occ
    block_w = max(band, 128)
    wide = states * rows
    loose = aux // 4 if aux * rows * virt * 2 > RESIDENT_BYTES else 0
    major = n_occ // (2 if n_occ % 2 == 0 else 1)
    dma = pltpu.SemaphoreType.DMA
    whole = pl.BlockSpec(memory_space=pl.ANY)
    densities = pl.pallas_call(
        functools.partial(densities_kernel, loose),
        out_shape=(
            jax.ShapeDtypeStruct((states, slab, band), F32),
            jax.ShapeDtypeStruct((states, rows, occ), F32),
            jax.ShapeDtypeStruct((states, rows, slab), F32),
        ),
        in_specs=[whole] * 2,
        out_specs=(whole,) * 3,
        scratch_shapes=[
            pltpu.VMEM((aux - loose, rows, virt), BF16),
            pltpu.VMEM((2, max(loose, 8), rows, n_aux * width), BF16),
            pltpu.VMEM((states, rows, virt), BF16),
            pltpu.VMEM((aux, wide), F32),
            pltpu.VMEM((states, aux // CHUNK, CHUNK * rows), F32),
            pltpu.VMEM((aux, CHUNK * rows), BF16),
            pltpu.VMEM((2, n_occ, states, aux), F32),
            pltpu.VMEM((wide, n_aux * width), F32),
            pltpu.VMEM((2, wide, width), F32),
            pltpu.VMEM((2, n_aux, wide, width), BF16),
            pltpu.VMEM((STAGES, n_aux, wide, width), BF16),
            pltpu.VMEM((states, occ, slab), BF16),
            pltpu.VMEM((states, occ, block_w), BF16),
            pltpu.VMEM((states, occ, slab), BF16),
            pltpu.VMEM((states, rows, occ), F32),
            pltpu.VMEM((n_aux, states, rows, occ // n_aux), F32),
            pltpu.VMEM((states, rows, occ), F32),
            pltpu.VMEM((states, rows, occ), F32),
            pltpu.VMEM((states, rows, occ), BF16),
            pltpu.VMEM((states, slab, band), F32),
            pltpu.VMEM((states, rows, slab), F32),
            dma((AHEAD,)),
            dma((2, n_aux)),
            dma((2 + states,)),
            dma((2, n_occ)),
            dma((2, n_occ)),
            dma((STAGES, n_aux)),
            dma((STAGES, n_aux)),
            dma((major,)),
            dma((major,)),
            dma((major,)),
            dma((major,)),
            dma((n_aux,)),
            dma(()),
            dma((STAGES, major)),
            dma((STAGES, major)),
            dma((STAGES, major)),
            dma((STAGES, major)),
            dma((n_aux,)),
            dma((n_aux,)),
            dma((n_aux,)),
            dma((n_aux,)),
            dma((n_aux,)),
            dma((n_aux,)),
        ],
        compiler_params=pltpu.CompilerParams(
            collective_id=0, has_side_effects=True, vmem_limit_bytes=67_043_328
        ),
        cost_estimate=pl.CostEstimate(
            flops=4 * wide * aux * rows * virt,
            bytes_accessed=2 * aux * rows * virt,
            transcendentals=0,
        ),
    )(amplitudes, factor)
    return write_results(*densities)


def solution(mesh):
    placed = (P(None, "occ", None), P("aux", "occ", None))
    return jax.shard_map(
        body,
        mesh=mesh,
        in_specs=placed,
        out_specs=(P(None, "aux", "occ"), P(None, "occ", None), P(None, "occ", "aux")),
        check_vma=False,
    )
```

```python
import functools

import jax
import jax.numpy as jnp
from jax import lax
from jax.experimental import pallas as pl
from jax.experimental.pallas import tpu as pltpu
from jax.sharding import PartitionSpec as P

F32 = jnp.float32
BF16 = jnp.bfloat16
NT = (((1,), (1,)), ((), ()))
TN = (((0,), (0,)), ((), ()))
MESH = pl.DeviceIdType.MESH
STAGES = 4
CHUNK = 16
FIT = 16
LOOSE_FIT = 32
AHEAD = 4
BATCH = 64
RESIDENT_BYTES = 52 << 20


def split3(value):
    hi = value.astype(BF16)
    rest = value - hi.astype(F32)
    mid = rest.astype(BF16)
    return hi, mid, (rest - mid.astype(F32)).astype(BF16)


def wide_dot(left, right):
    hi, mid, _ = split3(left)
    return jnp.dot(hi, right, preferred_element_type=F32) + jnp.dot(
        mid, right, preferred_element_type=F32
    )


def densities_kernel(
    loose, x_ref, b_ref, vd_ref, od_ref, rs_ref,
    held, spare, xv, sums, spread, sel, parts, acc, own, sent, got,
    xs, xb, fg, od_part, od_got, od, cross, cross_out, vd, rs,
    load_sem, spare_sem, local_sem, fit_send, fit_recv, part_send, part_recv,
    xa_send, xa_recv, xf_send, xf_recv, xb_send, xb_recv, fa_send, fa_recv, ff_send, ff_recv,
    or_send, or_recv, oa_send, oa_recv, cr_send, cr_recv,
):
    states, rows, virt = x_ref.shape
    aux = b_ref.shape[0]
    n_occ, n_aux = lax.axis_size("occ"), lax.axis_size("aux")
    me, aux_at = lax.axis_index("occ"), lax.axis_index("aux")
    minor = 2 if n_occ % 2 == 0 else 1
    major = n_occ // minor
    row_at, side = me // minor, lax.rem(me, minor)
    slab = virt // n_aux
    width = slab // STAGES
    band = virt // n_occ
    block_w = xb.shape[2]
    occ = xs.shape[1]
    piece_w = occ // n_aux
    kept = aux - loose
    kept_chunks = kept // FIT
    depth = CHUNK * rows
    wide = states * rows
    slab_at = pl.multiple_of(aux_at * slab, slab)

    def lines(o):
        return pl.ds(pl.multiple_of(o * rows, rows), rows)

    def occ_peer(d):
        return lax.rem(me + d, n_occ), aux_at

    def aux_peer(d):
        return me, lax.rem(aux_at + d, n_aux)

    def far(d):
        return lax.rem(row_at + d, major) * minor + side, aux_at

    def near():
        return row_at * minor + (minor - 1 - side), aux_at

    def from_far(d):
        return lax.rem(row_at + major - d, major) * minor + side

    def remote(src, dst, send, recv, to):
        return pltpu.make_async_remote_copy(
            src_ref=src, dst_ref=dst, send_sem=send, recv_sem=recv, device_id=to, device_id_type=MESH
        )

    def load(c):
        at = pl.ds(c * FIT, FIT)
        return pltpu.make_async_copy(b_ref.at[at], held.at[at], load_sem.at[c % AHEAD])

    def spare_loads(k):
        return [
            pltpu.make_async_copy(
                b_ref.at[pl.ds(kept, loose), :, pl.ds(u * slab + k * width, width)],
                spare.at[k % 2, :, :, pl.ds(u * width, width)],
                spare_sem.at[k % 2, u],
            )
            for u in range(n_aux)
        ]

    x_load = pltpu.make_async_copy(x_ref, xv, local_sem.at[0])
    own_cols = x_ref.at[:, :, pl.ds(slab_at, slab)]
    own_load = pltpu.make_async_copy(own_cols, xs.at[:, lines(me)], local_sem.at[1])
    x_load.start()
    ahead = min(AHEAD, kept_chunks)
    lead = 2 if loose else 0
    for c in range(lead or ahead):
        load(c).start()
    own_load.start()
    if loose:
        for k in (3, 2):
            for copy in spare_loads(k):
                copy.start()

    barrier = pltpu.get_barrier_semaphore()
    for d in range(1, n_occ):
        pl.semaphore_signal(barrier, inc=1, device_id=occ_peer(d), device_id_type=MESH)
    for d in range(1, n_aux):
        pl.semaphore_signal(barrier, inc=1, device_id=aux_peer(d), device_id_type=MESH)

    row = lax.broadcasted_iota(jnp.int32, (CHUNK, depth), 0)
    col = lax.broadcasted_iota(jnp.int32, (CHUNK, depth), 1)
    pattern = jnp.where(row == col // rows, 1.0, 0.0).astype(BF16)
    for n in range(aux // CHUNK):
        sel[n * CHUNK : (n + 1) * CHUNK] = pattern
    pl.semaphore_wait(barrier, n_occ + n_aux - 2)

    def x_far(d):
        return remote(own_cols, xs.at[:, lines(me)], xa_send.at[d], xa_recv.at[d], far(d))

    def x_far_got(d):
        at = xs.at[:, lines(from_far(d))]
        return remote(at, at, xa_send.at[d], xa_recv.at[d], far(d))

    def x_near(d):
        at = xs.at[:, lines(from_far(d))]
        return remote(at if d else own_cols, at, xf_send.at[d], xf_recv.at[d], near())

    for d in range(1, major):
        x_far(d).start()
    if minor > 1:
        x_near(0).start()

    def x_forward(d):
        x_far_got(d).wait_recv()
        if minor > 1:
            x_near(d).start()

    fit_line = lax.broadcasted_iota(jnp.int32, (rows, wide), 0)
    fit_lane = lax.broadcasted_iota(jnp.int32, (rows, wide), 1)
    same = (lax.rem(fit_lane, rows) == fit_line)[None]

    def pair_sums(block, left):
        pairs = lax.dot_general(
            block.reshape(block.shape[0] * rows, left.shape[1]), left, NT, preferred_element_type=F32
        )
        return jnp.sum(jnp.where(same, pairs.reshape(block.shape[0], rows, wide), 0.0), axis=1)

    def loose_fit(k):
        for copy in spare_loads(k):
            copy.wait()
        starts = [u * slab + k * width for u in range(n_aux)]

        def step(c, carry):
            left = jnp.concatenate([xv[:, :, a : a + width] for a in starts], axis=2)
            term = pair_sums(
                spare[k % 2, pl.ds(c * LOOSE_FIT, LOOSE_FIT)], left.reshape(wide, n_aux * width)
            )
            at = pl.ds(kept + c * LOOSE_FIT, LOOSE_FIT)
            if k == STAGES - 1:
                sums[at, :] = term
            else:
                sums[at, :] += term
            return carry

        lax.fori_loop(0, loose // LOOSE_FIT, step, 0)

    ind_row = lax.broadcasted_iota(jnp.int32, (8, wide), 0)
    ind_col = lax.broadcasted_iota(jnp.int32, (8, wide), 1)
    ind = jnp.where(ind_col // rows == ind_row, 1.0, 0.0).astype(BF16)
    spans = [(0, kept), (kept, loose)]

    def fit_copy(g, d):
        at = parts.at[g, me]
        return remote(at, at, fit_send.at[g, d], fit_recv.at[g, d], occ_peer(d))

    def send_fit(g):
        start, size = spans[g]
        pieces = split3(sums[start : start + size])
        fit = sum(lax.dot_general(ind, p, NT, preferred_element_type=F32) for p in pieces)
        parts[g, me] = jnp.zeros((states, aux), F32)
        parts[g, me, :, :size] = fit[:states]
        for d in range(1, n_occ):
            fit_copy(g, d).start()

    def spread_fit(g):
        start, size = spans[g]
        for d in range(1, n_occ):
            fit_copy(g, d).wait()
        total = parts[g, 0, :, :size]
        for j in range(1, n_occ):
            total += parts[g, j, :, :size]
        fitted = total.astype(BF16).astype(F32)
        chunks = size // CHUNK
        at_row = lax.broadcasted_iota(jnp.int32, (chunks, size), 0)
        at_col = lax.broadcasted_iota(jnp.int32, (chunks, size), 1)
        first = start // CHUNK
        for s in range(states):
            picked = jnp.where(
                at_col // CHUNK == at_row, jnp.broadcast_to(fitted[s : s + 1], (chunks, size)), 0.0
            )
            spread[s, first : first + chunks] = jnp.dot(
                picked.astype(BF16), sel[:size], preferred_element_type=F32
            )

    x_load.wait()
    def kept_sum(c):
        at = pl.ds(c * FIT, FIT)
        sums[at, :] = pair_sums(held[at], xv[...].reshape(wide, virt))

    def kept_fit(c, carry):
        load(c).wait()

        @pl.when(c + ahead < kept_chunks)
        def _():
            load(c + ahead).start()

        kept_sum(c)
        return carry

    def lead_fit(c, carry):
        load(c).wait()
        load(c + lead).start()
        kept_sum(c)
        return carry

    if loose:
        lax.fori_loop(0, lead, lead_fit, 0)
        for k in (3, 2):
            loose_fit(k)
            load(2 * lead + 3 - k).start()

    done = lead
    for d in range(1, major):
        upto = lead + (kept_chunks - lead) * d // major
        lax.fori_loop(done, upto, kept_fit, 0)
        done = upto
        x_forward(d)
    if loose:
        for k in (1, 0):
            for copy in spare_loads(k):
                copy.start()
    lax.fori_loop(done, kept_chunks, kept_fit, 0)
    send_fit(0)

    own_load.wait()
    if minor > 1:
        for d in range(major):
            x_near(d).wait_recv()
    for s in range(states):
        od_part[s] = lax.dot_general(xs[s, lines(me)], xs[s], NT, preferred_element_type=F32)

    def od_cols(u):
        return pl.ds(pl.multiple_of(u * piece_w, piece_w), piece_w)

    def od_reduce(d):
        to = aux_peer(d)
        return remote(od_part.at[:, :, od_cols(to[1])], od_got.at[d], or_send.at[d], or_recv.at[d], to)

    def od_share(d):
        at = od.at[:, :, od_cols(aux_at)]
        return remote(at, at, oa_send.at[d], oa_recv.at[d], aux_peer(d))

    for d in range(1, n_aux):
        od_reduce(d).start()

    holder = me * band // slab
    band_at = lax.rem(me * band, slab) // block_w * block_w
    band_cols = pl.ds(pl.multiple_of(band_at, block_w), block_w)
    mate = aux_at + 1 - 2 * lax.rem(aux_at, 2)
    along = lax.rem(aux_at, 2) == lax.rem(holder, 2)
    is_holder = aux_at == holder

    def band_copy(d, to):
        return remote(xs.at[:, :, band_cols], xb, xb_send.at[d], xb_recv, (me, to))

    relay = remote(xb, xb, xb_send.at[0], xb_recv, (me, mate))

    @pl.when(is_holder)
    def _():
        band_copy(0, mate).start()
        for d in range(2, n_aux, 2):
            band_copy(d, lax.rem(aux_at + d, n_aux)).start()
        xb[...] = xs[:, :, band_cols]

    if loose:
        for k in (1, 0):
            loose_fit(k)

    if loose:
        send_fit(1)

    spread_fit(0)
    lane = lax.broadcasted_iota(jnp.int32, (rows, depth), 1)
    line_at = lax.broadcasted_iota(jnp.int32, (rows, depth), 0)
    keep = lax.rem(lane, rows) == line_at

    def left_of(c):
        blocks = [
            jnp.concatenate(
                [
                    jnp.where(keep, jnp.broadcast_to(spread[s, pl.ds(q, 1)], (rows, depth)), 0.0)
                    for s in range(states)
                ],
                axis=0,
            ).astype(BF16)
            for q in [c * (BATCH // CHUNK) + n for n in range(BATCH // CHUNK)]
        ]
        return jnp.concatenate(blocks, axis=1)

    def part_copy(k, d):
        return remote(
            sent.at[k % 2, d], got.at[k, d], part_send.at[k, d], part_recv.at[k, d], aux_peer(d)
        )

    def piece_of(k, d):
        at = pl.multiple_of(lax.rem(aux_at + d, n_aux) * width, width)
        return acc[k % 2, :, pl.ds(at, width)]

    def f_at(o, k):
        return fg.at[:, lines(o), pl.ds(k * width, width)]

    def f_far(k, d):
        at = f_at(me, k)
        return remote(at, at, fa_send.at[k, d], fa_recv.at[k, d], far(d))

    def f_far_got(k, d):
        at = f_at(from_far(d), k)
        return remote(at, at, fa_send.at[k, d], fa_recv.at[k, d], far(d))

    def f_near(k, d):
        at = f_at(from_far(d), k)
        return remote(at, at, ff_send.at[k, d], ff_recv.at[k, d], near())

    def finish(k):
        for d in range(1, n_aux):
            part_copy(k, d).wait()
        value = own[k % 2]
        for d in range(1, n_aux):
            value += got[k, d].astype(F32)
        value = value.astype(BF16).reshape(states, rows, width)
        fg[:, lines(me), k * width : (k + 1) * width] = value
        for d in range(1, major):
            f_far(k, d).start()
        if minor > 1:
            f_near(k, 0).start()
        for s in range(states):
            term = lax.dot_general(
                value[s], xs[s, :, k * width : (k + 1) * width], NT, preferred_element_type=F32
            )
            if k:
                cross[s] += term
            else:
                cross[s] = term

    def forward(k):
        for d in range(1, major):
            f_far_got(k, d).wait_recv()
            if minor > 1:
                f_near(k, d).start()

    def share_od():
        for d in range(1, n_aux):
            od_reduce(d).wait()
        value = od_part[:, :, od_cols(aux_at)]
        for d in range(1, n_aux):
            value += od_got[d]
        od[:, :, od_cols(aux_at)] = value
        for d in range(1, n_aux):
            od_share(d).start()

    def kept_field(k):
        acc[k % 2] = jnp.zeros(acc.shape[1:], F32)

        def kept_step(c, carry):
            at = pl.ds(c * BATCH, BATCH)
            block = jnp.concatenate(
                [
                    held[at, :, u * slab + k * width : u * slab + (k + 1) * width].reshape(
                        BATCH * rows, width
                    )
                    for u in range(n_aux)
                ],
                axis=1,
            )
            acc[k % 2] += jnp.dot(left_of(c), block, preferred_element_type=F32)
            return carry

        lax.fori_loop(0, kept // BATCH, kept_step, 0)

    def loose_field(k):
        def loose_step(c, carry):
            block = spare[k % 2, pl.ds(c * BATCH, BATCH)].reshape(BATCH * rows, n_aux * width)
            acc[k % 2] += jnp.dot(left_of(kept // BATCH + c), block, preferred_element_type=F32)
            return carry

        lax.fori_loop(0, loose // BATCH, loose_step, 0)

    kept_field(0)
    kept_field(1)
    if loose:
        spread_fit(1)
    for k in range(STAGES):
        if k >= 2:
            kept_field(k)
        if loose:
            if k >= 2:
                for copy in spare_loads(k):
                    copy.wait()
            loose_field(k)
            if k < 2:
                for copy in spare_loads(k + 2):
                    copy.start()
        own[k % 2] = piece_of(k, 0)
        for d in range(1, n_aux):
            sent[k % 2, d] = piece_of(k, d).astype(BF16)
        for d in range(1, n_aux):
            part_copy(k, d).start()
        if k:
            finish(k - 1)
        if k == 1:
            share_od()
        if k == 2:

            @pl.when(jnp.logical_and(jnp.logical_not(is_holder), along))
            def _():
                relay.wait_recv()
                relay.start()

        if k >= 2:
            forward(k - 2)

    finish(STAGES - 1)

    def cross_got(d):
        return held.at[pl.ds(d * states, states), :, pl.ds(0, occ)]

    def cross_copy(d):
        return remote(cross_out, cross_got(d), cr_send.at[d], cr_recv.at[d], aux_peer(d))

    cross_out[...] = cross[...].astype(BF16)
    for d in range(1, n_aux):
        cross_copy(d).start()

    @pl.when(jnp.logical_not(along))
    def _():
        relay.wait_recv()

    vd_out = []
    for s in range(states):
        if s == 1:
            forward(STAGES - 2)

        def vd_step(n, carry, s=s):
            at = pl.ds(pl.multiple_of(n * 128, 128), 128)
            value = lax.dot_general(xs[s, :, at], xb[s], TN, preferred_element_type=F32)
            if block_w > band:
                off = lax.rem(me * band, block_w)
                picked = value[:, :band]
                for m in range(1, block_w // band):
                    picked = jnp.where(off == m * band, value[:, m * band : (m + 1) * band], picked)
                value = picked
            vd[s, at] = value
            return carry

        lax.fori_loop(0, slab // 128, vd_step, 0)
        vd_out.append(pltpu.make_async_copy(vd.at[s], vd_ref.at[s], local_sem.at[2 + s]))
        vd_out[-1].start()

    forward(STAGES - 1)
    for d in range(1, n_aux):
        od_share(d).wait()
    od_out = pltpu.make_async_copy(od, od_ref, local_sem.at[0])
    od_out.start()
    for d in range(1, n_aux):
        cross_copy(d).wait()
    for s in range(states):
        total = cross[s]
        for d in range(1, n_aux):
            total += held[d * states + s, :, :occ].astype(F32)
        rs[s] = wide_dot(total, xs[s])
    if minor > 1:
        for k in range(STAGES):
            for d in range(major):
                f_near(k, d).wait_recv()
    for s in range(states):
        rs[s] = rs[s] - wide_dot(od[s], fg[s])
    rs_out = pltpu.make_async_copy(rs, rs_ref, local_sem.at[1])
    rs_out.start()

    for d in range(1, major):
        x_far(d).wait_send()
        for k in range(STAGES):
            f_far(k, d).wait_send()
    if minor > 1:
        for d in range(major):
            x_near(d).wait_send()
            for k in range(STAGES):
                f_near(k, d).wait_send()

    @pl.when(is_holder)
    def _():
        band_copy(0, mate).wait_send()
        for d in range(2, n_aux, 2):
            band_copy(d, lax.rem(aux_at + d, n_aux)).wait_send()

    @pl.when(jnp.logical_and(jnp.logical_not(is_holder), along))
    def _():
        relay.wait_send()

    for copy in vd_out:
        copy.wait()
    od_out.wait()
    rs_out.wait()


def results_kernel(*refs):
    count = len(refs) // 3
    given, results, held = refs[:count], refs[count : 2 * count], refs[2 * count : 3 * count]
    sems = refs[3 * count]
    spans = [(n, s) for n in range(count) for s in range(given[n].shape[0])]
    ins, outs = [], []
    for at, (n, s) in enumerate(spans):
        ins.append(pltpu.make_async_copy(given[n].at[s], held[n].at[s], sems.at[at, 0]))
        outs.append(pltpu.make_async_copy(held[n].at[s], results[n].at[s], sems.at[at, 1]))
    for copy in ins:
        copy.start()
    for at in range(len(spans)):
        ins[at].wait()
        outs[at].start()
    for copy in outs:
        copy.wait()


def write_results(*given):
    whole = pl.BlockSpec(memory_space=pl.ANY)
    count = len(given)
    return pl.pallas_call(
        results_kernel,
        out_shape=tuple(jax.ShapeDtypeStruct(g.shape, g.dtype) for g in given),
        in_specs=[whole] * count,
        out_specs=(whole,) * count,
        scratch_shapes=[
            *[pltpu.VMEM(g.shape, g.dtype) for g in given],
            pltpu.SemaphoreType.DMA((sum(g.shape[0] for g in given), 2)),
        ],
        cost_estimate=pl.CostEstimate(
            flops=0, bytes_accessed=2 * sum(g.size * 4 for g in given), transcendentals=0
        ),
    )(*given)


def body(amplitudes, factor):
    n_occ, n_aux = lax.axis_size("occ"), lax.axis_size("aux")
    states, rows, virt = amplitudes.shape
    aux = factor.shape[0]
    occ = rows * n_occ
    slab = virt // n_aux
    width = slab // STAGES
    band = virt // n_occ
    block_w = max(band, 128)
    wide = states * rows
    loose = aux // 4 if aux * rows * virt * 2 > RESIDENT_BYTES else 0
    major = n_occ // (2 if n_occ % 2 == 0 else 1)
    dma = pltpu.SemaphoreType.DMA
    whole = pl.BlockSpec(memory_space=pl.ANY)
    densities = pl.pallas_call(
        functools.partial(densities_kernel, loose),
        out_shape=(
            jax.ShapeDtypeStruct((states, slab, band), F32),
            jax.ShapeDtypeStruct((states, rows, occ), F32),
            jax.ShapeDtypeStruct((states, rows, slab), F32),
        ),
        in_specs=[whole] * 2,
        out_specs=(whole,) * 3,
        scratch_shapes=[
            pltpu.VMEM((aux - loose, rows, virt), BF16),
            pltpu.VMEM((2, max(loose, 8), rows, n_aux * width), BF16),
            pltpu.VMEM((states, rows, virt), BF16),
            pltpu.VMEM((aux, wide), F32),
            pltpu.VMEM((states, aux // CHUNK, CHUNK * rows), F32),
            pltpu.VMEM((aux, CHUNK * rows), BF16),
            pltpu.VMEM((2, n_occ, states, aux), F32),
            pltpu.VMEM((2, wide, n_aux * width), F32),
            pltpu.VMEM((2, wide, width), F32),
            pltpu.VMEM((2, n_aux, wide, width), BF16),
            pltpu.VMEM((STAGES, n_aux, wide, width), BF16),
            pltpu.VMEM((states, occ, slab), BF16),
            pltpu.VMEM((states, occ, block_w), BF16),
            pltpu.VMEM((states, occ, slab), BF16),
            pltpu.VMEM((states, rows, occ), F32),
            pltpu.VMEM((n_aux, states, rows, occ // n_aux), F32),
            pltpu.VMEM((states, rows, occ), F32),
            pltpu.VMEM((states, rows, occ), F32),
            pltpu.VMEM((states, rows, occ), BF16),
            pltpu.VMEM((states, slab, band), F32),
            pltpu.VMEM((states, rows, slab), F32),
            dma((AHEAD,)),
            dma((2, n_aux)),
            dma((2 + states,)),
            dma((2, n_occ)),
            dma((2, n_occ)),
            dma((STAGES, n_aux)),
            dma((STAGES, n_aux)),
            dma((major,)),
            dma((major,)),
            dma((major,)),
            dma((major,)),
            dma((n_aux,)),
            dma(()),
            dma((STAGES, major)),
            dma((STAGES, major)),
            dma((STAGES, major)),
            dma((STAGES, major)),
            dma((n_aux,)),
            dma((n_aux,)),
            dma((n_aux,)),
            dma((n_aux,)),
            dma((n_aux,)),
            dma((n_aux,)),
        ],
        compiler_params=pltpu.CompilerParams(
            collective_id=0, has_side_effects=True, vmem_limit_bytes=67_043_328
        ),
        cost_estimate=pl.CostEstimate(
            flops=4 * wide * aux * rows * virt,
            bytes_accessed=2 * aux * rows * virt,
            transcendentals=0,
        ),
    )(amplitudes, factor)
    return write_results(*densities)


def solution(mesh):
    placed = (P(None, "occ", None), P("aux", "occ", None))
    return jax.shard_map(
        body,
        mesh=mesh,
        in_specs=placed,
        out_specs=(P(None, "aux", "occ"), P(None, "occ", None), P(None, "occ", "aux")),
        check_vma=False,
    )
```
